128 devices in a mesh: row: 16 (over x, z_lo, core), col: 8 (over z_hi, y).
Axes of the slice: x: 4, y: 4, z: 4 (z_hi: 2, z_lo: 2; z = z_hi * 2 + z_lo), core: 2. Of those that a mesh axis runs over, the one named last changes fastest.
Arguments:
- value_proj: float32 [16, 8, 1024, 512], P('row', 'col'), may hold values from -6 to 6
- token_pool: bfloat16 [16, 8, 1536, 1024], P('row', 'col'), may hold values from -6 to 6
- target_pool: bfloat16 [16, 8, 1536, 1024], P('row', 'col'), may hold values from -6 to 6
- batch_ids: int32 [16, 8, 3, 1536], P('row', 'col'), may hold values from 0 to 1535
- frozen_out: bfloat16 [512, 1024], replicated, may hold values from -0.25 to 0.25
- numerators: int32 [3], replicated, may hold values from 4 to 15
Outputs:
- final_proj: float32 [16, 8, 1024, 512], P('row', 'col')
- final_tracker: float32 [16, 8, 1024, 512], P('row', 'col')
The draws below stay inside these ranges and needn't reach their ends.
All inputs are finite; a program needn't handle non-finite values.
Results may differ from the reference program's by a relative error of at most 0.017.
Values sent between devices are 32-bit elements; how exact they have to be, the bound alone decides.
A program may use at most 128 MiB of HBM per device.

```python
import jax
import jax.numpy as jnp
from jax import lax

D = 1024
HD = 512
BATCH = 1536
ITERS = 2
POOL = 1536
N_ROW = 16
N_COL = 8


def plant(drawn, stream_key, low, high):
    longest = drawn.shape.index(max(drawn.shape))
    spots = []
    for shift in (0, 1):
        where = [jax.random.randint(jax.random.fold_in(stream_key, axis), (), 0, length) for axis, length in enumerate(drawn.shape)]
        where[longest] = (where[longest] + shift) % drawn.shape[longest]
        spots.append(tuple(where))
    return drawn.at[spots[0]].set(low).at[spots[1]].set(high)


def steps_of(stream_key, shape, split, least, top_value):
    level, own = 1.0, jax.random.fold_in(stream_key, 6)
    for dim, parts in split:
        draws = jnp.exp(jax.random.uniform(jax.random.fold_in(own, dim), (parts,), jnp.float32, least / len(split), top_value / len(split)))
        level = level * jnp.repeat(draws, shape[dim] // parts).reshape([-1 if axis == dim else 1 for axis in range(len(shape))])
    return level


def normal_values(key, dims, width, reach, pieces=(), held_as=jnp.bfloat16):
    values = width * jax.random.normal(key, dims, jnp.float32)
    if pieces:
        values = values * steps_of(key, dims, pieces, -0.22, 0.18)
    return jnp.clip(values, -reach, reach).astype(held_as)


def setup_inputs(seed: int = 0) -> dict:
    streams_of = jax.random.split(jax.random.key(seed), 7)
    return {
        "value_proj": normal_values(streams_of[0], (N_ROW, N_COL, D, HD), 1.0, 6.0, ((0, 16), (1, 8)), jnp.float32),
        "token_pool": normal_values(streams_of[1], (N_ROW, N_COL, POOL, D), 1.0, 6.0, ((0, 16), (1, 8))),
        "target_pool": normal_values(streams_of[2], (N_ROW, N_COL, POOL, D), 1.0, 6.0, ((0, 16), (1, 8))),
        "batch_ids": plant(jax.random.randint(streams_of[3], (N_ROW, N_COL, ITERS + 1, BATCH), 0, POOL), jax.random.fold_in(streams_of[3], 1), 0, POOL - 1).astype(jnp.int32),
        "frozen_out": normal_values(streams_of[4], (HD, D), HD ** -0.5, 0.25),
        "numerators": jax.random.randint(streams_of[5], (3,), 4, 16).astype(jnp.int32),
    }


step_rate = 0.2


def grad_single(current, pool_rows, target_rows, chosen, frozen_out):
    factor = D ** -0.5
    tokens = pool_rows[chosen]
    targets = target_rows[chosen]
    preact = jnp.dot(tokens, current.astype(jnp.bfloat16), preferred_element_type=jnp.float32) * factor
    sigmoid_pre = jax.nn.sigmoid(preact)
    hidden = (preact * sigmoid_pre).astype(jnp.bfloat16)
    output = jnp.dot(hidden, frozen_out, preferred_element_type=jnp.float32)
    error_term = (output - targets.astype(jnp.float32)).astype(jnp.bfloat16)
    back_hidden = lax.dot_general(error_term, frozen_out, (((1,), (1,)), ((), ())), preferred_element_type=jnp.float32)
    slope = sigmoid_pre * (1.0 + preact * (1.0 - sigmoid_pre))
    back_pre = (back_hidden * slope).astype(jnp.bfloat16)
    return lax.dot_general(tokens, back_pre, (((0,), (0,)), ((), ())), preferred_element_type=jnp.float32) * factor


def all_gradients(current, token_pool, target_pool, batch_ids, frozen_out, which):
    count = N_ROW * N_COL

    def flatten(array):
        return array.reshape((count,) + array.shape[2:])

    def single(items):
        return grad_single(items[0], items[1], items[2], items[3], frozen_out)

    result = lax.map(single, (flatten(current), flatten(token_pool), flatten(target_pool), flatten(batch_ids[:, :, which])))
    return result.reshape(current.shape)


def gossip(field, mix_weights):
    return mix_weights[0] * field + mix_weights[1] * jnp.roll(field, 1, 0) + mix_weights[2] * jnp.roll(field, 1, 1)


def reference(value_proj, token_pool, target_pool, batch_ids, frozen_out, numerators):
    counts = numerators.astype(jnp.float32)
    mix_weights = counts / jnp.sum(counts)
    current = value_proj
    grad_old = all_gradients(current, token_pool, target_pool, batch_ids, frozen_out, 0)
    tracker = grad_old
    for which in range(1, ITERS + 1):
        current_new = gossip(current, mix_weights) - step_rate * tracker
        grad_new = all_gradients(current_new, token_pool, target_pool, batch_ids, frozen_out, which)
        tracker = (gossip(tracker, mix_weights) + grad_new) - grad_old
        current = current_new
        grad_old = grad_new
    return current, tracker
```

```python
import functools

import jax
import jax.numpy as jnp
from jax import lax
from jax.experimental import pallas as pl
from jax.experimental.pallas import tpu as pltpu
from jax.sharding import PartitionSpec as P

MESH = pl.DeviceIdType.MESH
F32 = jnp.float32
BF16 = jnp.bfloat16
STEP = 0.2
LANES = 128
TILE = 256


def kernel(
    num_ref, x_hbm, tok_hbm, tgt_hbm, ids_ref, fro_hbm,
    xo_hbm, to_hbm,
    xs, xr, xc, xa, xx, ws, wr, g0, gr, gc, g1, ts, tr, tc, q, g2,
    x_relay, g_relay, t_relay,
    tok, tgt, tokt, fro, frot, bp, xb,
    load_sem, x_sem, out_sem,
    xr_s, xr_r, xc_s, xc_r, xa_s, xa_r, xx_s, xx_r, wr_s, wr_r,
    gr_s, gr_r, gc_s, gc_r, tr_s, tr_r, tc_s, tc_r,
    rel_s, rel_r,
):
    chunks, rows, _ = xs.shape
    n_pool, depth = tok.shape
    heads = fro.shape[0]
    factor = depth ** -0.5

    r, c = lax.axis_index("row"), lax.axis_index("col")
    y, half = lax.rem(c, 4), 4 * (c // 4)
    seam = y == 3
    row_next = (lax.rem(r + 1, 16), c)
    row_prev = (lax.rem(r + 15, 16), c)
    col_next = (r, lax.rem(c + 1, 8))
    swap = (r, lax.rem(c + 4, 8))
    up = (r, half + lax.rem(y + 1, 4))
    down = (r, half + lax.rem(y + 3, 4))
    up_swap = (r, lax.rem(up[1] + 4, 8))
    down_swap = (r, lax.rem(down[1] + 4, 8))
    two_first = (r, jnp.where(y >= 2, down_swap[1], down[1]))

    loads = [
        pltpu.make_async_copy(x_hbm.at[0, 0, :, pl.ds(i * LANES, LANES)], xs.at[i], x_sem.at[i])
        for i in range(chunks)
    ]
    for load in loads:
        load.start()
    tok_load = pltpu.make_async_copy(tok_hbm.at[0, 0], tok, load_sem.at[0])
    fro_load = pltpu.make_async_copy(fro_hbm, fro, load_sem.at[1])
    tgt_load = pltpu.make_async_copy(tgt_hbm.at[0, 0], tgt, load_sem.at[2])
    tok_load.start()
    fro_load.start()
    tgt_load.start()

    barrier = pltpu.get_barrier_semaphore()
    partners = (row_next, row_prev, up, down, swap, up_swap, down_swap)
    for partner in partners:
        pl.semaphore_signal(barrier, inc=1, device_id=partner, device_id_type=MESH)
    pl.semaphore_wait(barrier, len(partners))

    def remote(src, dst, send, recv, i, device, j=None):
        return pltpu.make_async_remote_copy(
            src_ref=src.at[i], dst_ref=dst.at[i if j is None else j], send_sem=send.at[i],
            recv_sem=recv.at[i], device_id=device, device_id_type=MESH,
        )

    def relayed(i):
        return i % 2 == 1

    def swap_copy(src, relay, which, send, i):
        return pltpu.make_async_remote_copy(
            src_ref=src.at[i], dst_ref=relay.at[i // 2], send_sem=send.at[i],
            recv_sem=rel_r.at[which, i // 2], device_id=swap, device_id_type=MESH,
        )

    def forward_copy(relay, which, dst, recv, i):
        return pltpu.make_async_remote_copy(
            src_ref=relay.at[i // 2], dst_ref=dst.at[i], send_sem=rel_s.at[which, i // 2],
            recv_sem=recv.at[i], device_id=up, device_id_type=MESH,
        )

    def send_swaps(src, relay, which, send, i):
        if relayed(i):
            @pl.when(seam)
            def _():
                swap_copy(src, relay, which, send, i).start()

    def send_col(src, dst, send, recv, i):
        copy = remote(src, dst, send, recv, i, col_next)
        if relayed(i):
            pl.when(jnp.logical_not(seam))(copy.start)
        else:
            copy.start()

    def forward(src, relay, which, dst, send, recv, i):
        if relayed(i):
            @pl.when(seam)
            def _():
                swap_copy(src, relay, which, send, i).wait_recv()
                forward_copy(relay, which, dst, recv, i).start()

    for i in range(chunks):
        loads[i].wait()
        send_swaps(xs, x_relay, 0, xc_s, i)
        send_col(xs, xc, xc_s, xc_r, i)
    for i in range(chunks):
        remote(xs, xr, xr_s, xr_r, i, row_next).start()
    for i in range(chunks):
        remote(xs, xa, xa_s, xa_r, i, two_first).start()

    weights = [jnp.full((1, LANES), num_ref[i].astype(F32), F32) for i in range(3)]
    total = weights[0] + weights[1] + weights[2]
    own, by_row, by_col = (w / total for w in weights)

    def over(i, body):
        def step(t, carry):
            body(pl.ds(pl.multiple_of(t * LANES, LANES), LANES))
            return carry

        lax.fori_loop(0, rows // LANES, step, 0)

    def gradient(which, out):
        def tile(t, carry):
            at = pl.ds(pl.multiple_of(t * TILE, TILE), TILE)
            pre = jnp.dot(tok[at, :], xb[...], preferred_element_type=F32) * factor
            sig = jax.nn.sigmoid(pre)
            hidden = (pre * sig).astype(BF16)
            slope = sig * (1.0 + pre * (1.0 - sig))
            output = jnp.dot(hidden, fro[...], preferred_element_type=F32)
            err = (output - tgt[at, :].astype(F32)).astype(BF16)
            back = jnp.dot(err, frot[...], preferred_element_type=F32)
            place = t * TILE + lax.broadcasted_iota(jnp.int32, (TILE, LANES), 0)
            drawn = jnp.zeros((TILE, LANES), F32)
            for l in range(ids_ref.shape[3] // LANES):
                ids = ids_ref[0, 0, which : which + 1, l * LANES : (l + 1) * LANES]
                drawn += jnp.where(ids == place, 1.0, 0.0)
            drawn = jnp.sum(drawn, axis=1, keepdims=True)
            bp[at, :] = (back * slope * drawn).astype(BF16)
            return carry

        lax.fori_loop(0, n_pool // TILE, tile, 0)

        def block(t, carry):
            at = pl.ds(pl.multiple_of(t * TILE, TILE), TILE)
            for n in range(heads // TILE):
                g = jnp.dot(tokt[at, :], bp[:, n * TILE : (n + 1) * TILE], preferred_element_type=F32) * factor
                for l in range(TILE // LANES):
                    out[n * (TILE // LANES) + l, at, :] = g[:, l * LANES : (l + 1) * LANES]
            return carry

        lax.fori_loop(0, depth // TILE, block, 0)

    def cols(i):
        return slice(i * LANES, (i + 1) * LANES)

    for i in range(chunks):
        def cast(at, i=i):
            xb[at, cols(i)] = xs[i, at, :].astype(BF16)
        over(i, cast)
    tok_load.wait()

    def turn(t, carry):
        at = pl.ds(pl.multiple_of(t * TILE, TILE), TILE)
        tokt[:, at] = tok[at, :].T
        return carry

    lax.fori_loop(0, n_pool // TILE, turn, 0)
    fro_load.wait()
    for t in range(heads // TILE):
        frot[:, t * TILE : (t + 1) * TILE] = fro[t * TILE : (t + 1) * TILE, :].T
    tgt_load.wait()
    gradient(0, g0)

    for i in range(chunks):
        send_swaps(g0, g_relay, 1, gc_s, i)
    for i in range(chunks):
        remote(g0, gr, gr_s, gr_r, i, row_next).start()
    for i in range(chunks):
        forward(xs, x_relay, 0, xc, xc_s, xc_r, i)
    for i in range(chunks):
        send_col(g0, gc, gc_s, gc_r, i)

    def pass_on(i):
        remote(xs, xa, xa_s, xa_r, i, two_first).wait_recv()
        remote(xa, xx, xx_s, xx_r, i, down).start()

    for i in range(chunks // 2):
        pass_on(i)

    for i in range(chunks):
        remote(xs, xc, xc_s, xc_r, i, col_next).wait_recv()
        remote(xs, xr, xr_s, xr_r, i, row_next).wait_recv()

        def first(at, i=i):
            from_col = by_col * xc[i, at, :]
            mixed = own * xs[i, at, :] + by_row * xr[i, at, :] + from_col
            ws[i, at, :] = mixed + from_col
            xb[at, cols(i)] = (mixed - STEP * g0[i, at, :]).astype(BF16)

        over(i, first)
        remote(ws, wr, wr_s, wr_r, i, row_next).start()
    gradient(1, g1)

    for i in range(chunks // 2, chunks):
        pass_on(i)
    for i in range(chunks):
        forward(g0, g_relay, 1, gc, gc_s, gc_r, i)

    for i in range(chunks):
        remote(g0, gc, gc_s, gc_r, i, col_next).wait_recv()
        remote(g0, gr, gr_s, gr_r, i, row_next).wait_recv()

        def second(at, i=i):
            g = g0[i, at, :]
            mixed = own * g + by_row * gr[i, at, :] + by_col * gc[i, at, :]
            track = (mixed + g1[i, at, :]) - g
            ts[i, at, :] = track
            q[i, at, :] = STEP * (mixed + track)

        over(i, second)
        send_swaps(ts, t_relay, 2, tc_s, i)
        send_col(ts, tc, tc_s, tc_r, i)
        remote(ts, tr, tr_s, tr_r, i, row_next).start()

    outs = []
    for i in range(chunks):
        remote(ws, wr, wr_s, wr_r, i, row_next).wait_recv()
        remote(xa, xx, xx_s, xx_r, i, down).wait_recv()

        def third(at, i=i):
            new = own * ws[i, at, :] + by_row * wr[i, at, :] + (by_col * by_col) * xx[i, at, :] - q[i, at, :]
            q[i, at, :] = new
            xb[at, cols(i)] = new.astype(BF16)

        over(i, third)
        out = pltpu.make_async_copy(q.at[i], xo_hbm.at[0, 0, :, pl.ds(i * LANES, LANES)], out_sem.at[0, i])
        out.start()
        outs.append(out)
    gradient(2, g2)

    for i in range(chunks):
        forward(ts, t_relay, 2, tc, tc_s, tc_r, i)

    for i in range(chunks):
        remote(ts, tc, tc_s, tc_r, i, col_next).wait_recv()
        remote(ts, tr, tr_s, tr_r, i, row_next).wait_recv()

        def last(at, i=i):
            mixed = own * ts[i, at, :] + by_row * tr[i, at, :] + by_col * tc[i, at, :]
            g2[i, at, :] = (mixed + g2[i, at, :]) - g1[i, at, :]

        over(i, last)
        out = pltpu.make_async_copy(g2.at[i], to_hbm.at[0, 0, :, pl.ds(i * LANES, LANES)], out_sem.at[1, i])
        out.start()
        outs.append(out)

    for i in range(chunks):
        remote(xs, xc, xc_s, xc_r, i, col_next).wait_send()
        remote(xs, xr, xr_s, xr_r, i, row_next).wait_send()
        remote(xs, xa, xa_s, xa_r, i, two_first).wait_send()
        remote(xa, xx, xx_s, xx_r, i, down).wait_send()
        remote(ws, wr, wr_s, wr_r, i, row_next).wait_send()
        remote(g0, gc, gc_s, gc_r, i, col_next).wait_send()
        remote(g0, gr, gr_s, gr_r, i, row_next).wait_send()
        remote(ts, tc, tc_s, tc_r, i, col_next).wait_send()
        remote(ts, tr, tr_s, tr_r, i, row_next).wait_send()
        if relayed(i):
            @pl.when(seam)
            def _():
                forward_copy(x_relay, 0, xc, xc_r, i).wait_send()
                forward_copy(g_relay, 1, gc, gc_r, i).wait_send()
                forward_copy(t_relay, 2, tc, tc_r, i).wait_send()
    for out in outs:
        out.wait()


def on_device(value_proj, token_pool, target_pool, batch_ids, frozen_out, numerators):
    depth, heads = value_proj.shape[2:]
    n_pool = token_pool.shape[2]
    chunks = heads // LANES
    field = pltpu.VMEM((chunks, depth, LANES), F32)
    relay = pltpu.VMEM((chunks // 2, depth, LANES), F32)
    dma = pltpu.SemaphoreType.DMA
    out = jax.ShapeDtypeStruct(value_proj.shape, F32)
    hbm = pl.BlockSpec(memory_space=pl.ANY)
    return pl.pallas_call(
        kernel,
        out_shape=(out, out),
        in_specs=[
            pl.BlockSpec(memory_space=pltpu.SMEM), hbm, hbm, hbm,
            pl.BlockSpec(memory_space=pltpu.VMEM), hbm,
        ],
        out_specs=(hbm, hbm),
        scratch_shapes=[field] * 16 + [relay] * 3 + [
            pltpu.VMEM((n_pool, depth), BF16),
            pltpu.VMEM((n_pool, depth), BF16),
            pltpu.VMEM((depth, n_pool), BF16),
            pltpu.VMEM((heads, depth), BF16),
            pltpu.VMEM((depth, heads), BF16),
            pltpu.VMEM((n_pool, heads), BF16),
            pltpu.VMEM((depth, heads), BF16),
            dma((3,)), dma((chunks,)), dma((2, chunks)),
        ] + [dma((chunks,))] * 18 + [dma((3, chunks // 2))] * 2,
        compiler_params=pltpu.CompilerParams(
            collective_id=0, has_side_effects=True, vmem_limit_bytes=67043328,
        ),
    )(numerators, value_proj, token_pool, target_pool, batch_ids, frozen_out)


def solution(mesh):
    return jax.shard_map(
        on_device,
        mesh=mesh,
        in_specs=(
            P("row", "col", None, None),
            P("row", "col", None, None),
            P("row", "col", None, None),
            P("row", "col", None, None),
            P(),
            P(),
        ),
        out_specs=(P("row", "col", None, None), P("row", "col", None, None)),
        check_vma=False,
    )
```

```python
import functools

import jax
import jax.numpy as jnp
from jax import lax
from jax.experimental import pallas as pl
from jax.experimental.pallas import tpu as pltpu
from jax.sharding import PartitionSpec as P

MESH = pl.DeviceIdType.MESH
F32 = jnp.float32
BF16 = jnp.bfloat16
STEP = 0.2
SPLIT = 2
LANES = 128
TILE = 256


def kernel(
    num_ref, x_hbm, tok_hbm, tgt_hbm, ids_hbm, fro_hbm,
    xo, to,
    xs, xr, xc, xa, xx, ws, wr, g0, gr, gc, g1, ts, tr, tc, q,
    x_relay, g_relay, t_relay,
    tok, tgt, tokt, fro, frot, bp, xb, ids_ref,
    load_sem, x_sem,
    xr_s, xr_r, xc_s, xc_r, xa_s, xa_r, xx_s, xx_r, wr_s, wr_r,
    gr_s, gr_r, gc_s, gc_r, tr_s, tr_r, tc_s, tc_r,
    rel_s, rel_r,
):
    chunks, rows, _ = xs.shape
    split = tok.shape[1] // rows
    scope = jax.named_scope
    n_pool, depth = tok.shape
    heads = fro.shape[0]
    factor = depth ** -0.5

    r, c = lax.axis_index("row"), lax.axis_index("col")
    y, half = lax.rem(c, 4), 4 * (c // 4)
    seam = y == 3
    plain = jnp.logical_not(seam)
    inner = jnp.logical_or(y == 1, y == 2)
    outer = jnp.logical_not(inner)
    through = jnp.logical_and(seam, lax.rem(r, 4) >= 2)
    landing = y == 0
    direct = jnp.logical_and(seam, jnp.logical_not(through))
    row_next = (lax.rem(r + 1, 16), c)
    row_prev = (lax.rem(r + 15, 16), c)
    col_next = (r, lax.rem(c + 1, 8))
    swap = (r, lax.rem(c + 4, 8))
    up = (r, half + lax.rem(y + 1, 4))
    down = (r, half + lax.rem(y + 3, 4))
    up_swap = (r, lax.rem(up[1] + 4, 8))
    down_swap = (r, lax.rem(down[1] + 4, 8))
    two_first = (r, jnp.where(y >= 2, down_swap[1], down[1]))

    def window(ref, i):
        return ref.at[0, 0, pl.ds((i % split) * rows, rows), pl.ds((i // split) * LANES, LANES)]

    loads = [
        pltpu.make_async_copy(window(x_hbm, i), xs.at[i], x_sem.at[i])
        for i in range(chunks)
    ]
    for load in loads:
        load.start()
    tok_load = pltpu.make_async_copy(tok_hbm.at[0, 0], tok, load_sem.at[0])
    fro_load = pltpu.make_async_copy(fro_hbm, fro, load_sem.at[1])
    tgt_load = pltpu.make_async_copy(tgt_hbm.at[0, 0], tgt, load_sem.at[2])
    ids_load = pltpu.make_async_copy(ids_hbm, ids_ref, load_sem.at[3])
    ids_load.start()
    tok_load.start()
    fro_load.start()
    tgt_load.start()

    barrier = pltpu.get_barrier_semaphore()
    partners = (row_next, row_prev, up, down, swap, up_swap, down_swap)
    for partner in partners:
        pl.semaphore_signal(barrier, inc=1, device_id=partner, device_id_type=MESH)
    pl.semaphore_wait(barrier, len(partners))

    def remote(src, dst, send, recv, i, device, j=None):
        return pltpu.make_async_remote_copy(
            src_ref=src.at[i], dst_ref=dst.at[i if j is None else j], send_sem=send.at[i],
            recv_sem=recv.at[i], device_id=device, device_id_type=MESH,
        )

    def relayed(i):
        return i % 2 == 1

    def swap_copy(src, relay, which, send, i):
        return pltpu.make_async_remote_copy(
            src_ref=src.at[i], dst_ref=relay.at[i // 2], send_sem=send.at[i],
            recv_sem=rel_r.at[which, i // 2], device_id=swap, device_id_type=MESH,
        )

    def forward_copy(relay, which, dst, recv, i):
        return pltpu.make_async_remote_copy(
            src_ref=relay.at[i // 2], dst_ref=dst.at[i], send_sem=rel_s.at[which, i // 2],
            recv_sem=recv.at[i], device_id=up, device_id_type=MESH,
        )

    def send_swaps(src, relay, which, send, i):
        if relayed(i):
            @pl.when(seam)
            def _():
                swap_copy(src, relay, which, send, i).start()

    def send_col(src, dst, send, recv, i):
        copy = remote(src, dst, send, recv, i, col_next)
        if relayed(i):
            pl.when(jnp.logical_not(seam))(copy.start)
        else:
            copy.start()

    def forward(src, relay, which, dst, send, recv, i):
        if relayed(i):
            @pl.when(seam)
            def _():
                swap_copy(src, relay, which, send, i).wait_recv()
                forward_copy(relay, which, dst, recv, i).start()

    for i in range(chunks):
        loads[i].wait()
        send_swaps(xs, x_relay, 0, xc_s, i)
        send_col(xs, xc, xc_s, xc_r, i)
    def send_rows(src, dst, send, recv, condition=None):
        def go():
            for i in range(chunks):
                remote(src, dst, send, recv, i, row_next).start()

        if condition is None:
            go()
        else:
            pl.when(condition)(go)

    def early(src, dst, send, recv):
        @pl.when(landing)
        def _():
            for i in range(chunks):
                if not relayed(i):
                    remote(src, dst, send, recv, i, col_next).wait_recv()

    def wait_col(src, dst, send, recv, i):
        wait = remote(src, dst, send, recv, i, col_next).wait_recv
        if relayed(i):
            wait()
        else:
            pl.when(jnp.logical_not(landing))(wait)

    send_rows(xs, xr, xr_s, xr_r, jnp.logical_or(inner, direct))
    for i in range(chunks):
        remote(xs, xa, xa_s, xa_r, i, two_first).start()

    weights = [jnp.full((1, LANES), num_ref[i].astype(F32), F32) for i in range(3)]
    total = weights[0] + weights[1] + weights[2]
    own, by_row, by_col = (w / total for w in weights)

    def over(i, body):
        def step(t, carry):
            body(pl.ds(pl.multiple_of(t * LANES, LANES), LANES))
            return carry

        lax.fori_loop(0, rows // LANES, step, 0)

    def gradient(which, out):
        def tile(t, carry):
            at = pl.ds(pl.multiple_of(t * TILE, TILE), TILE)
            pre = jnp.dot(tok[at, :], xb[...], preferred_element_type=F32) * factor
            sig = jax.nn.sigmoid(pre)
            hidden = (pre * sig).astype(BF16)
            slope = sig * (1.0 + pre * (1.0 - sig))
            output = jnp.dot(hidden, fro[...], preferred_element_type=F32)
            err = (output - tgt[at, :].astype(F32)).astype(BF16)
            back = jnp.dot(err, frot[...], preferred_element_type=F32)
            place = t * TILE + lax.broadcasted_iota(jnp.int32, (TILE, LANES), 0)
            drawn = jnp.zeros((TILE, LANES), F32)
            for l in range(ids_ref.shape[2] // LANES):
                ids = ids_ref[which, :, l * LANES : (l + 1) * LANES]
                drawn += jnp.where(ids == place, 1.0, 0.0)
            drawn = jnp.sum(drawn, axis=1, keepdims=True)
            bp[at, :] = (back * slope * drawn).astype(BF16)
            return carry

        lax.fori_loop(0, n_pool // TILE, tile, 0)

        def block(t, carry):
            to = pl.ds(pl.multiple_of(t * TILE, TILE), TILE)
            for p in range(split):
                at = pl.ds(pl.multiple_of(t * TILE + p * rows, TILE), TILE)
                for n in range(heads // TILE):
                    g = jnp.dot(tokt[at, :], bp[:, n * TILE : (n + 1) * TILE], preferred_element_type=F32) * factor
                    for l in range(TILE // LANES):
                        out[(n * (TILE // LANES) + l) * split + p, to, :] = g[:, l * LANES : (l + 1) * LANES]
            return carry

        lax.fori_loop(0, rows // TILE, block, 0)

    def store(ref, i, at, value):
        to_rows = pl.ds(at.start + (i % split) * rows, LANES)
        ref[0, 0, to_rows, (i // split) * LANES : (i // split + 1) * LANES] = value

    def put(i, at, value):
        to = pl.ds(at.start + (i % split) * rows, LANES)
        xb[to, (i // split) * LANES : (i // split + 1) * LANES] = value.astype(BF16)

    for i in range(chunks):
        def cast(at, i=i):
            put(i, at, xs[i, at, :])
        over(i, cast)
    tok_load.wait()

    def turn(t, carry):
        at = pl.ds(pl.multiple_of(t * TILE, TILE), TILE)
        tokt[:, at] = tok[at, :].T
        return carry

    lax.fori_loop(0, n_pool // TILE, turn, 0)
    fro_load.wait()
    for t in range(heads // TILE):
        frot[:, t * TILE : (t + 1) * TILE] = fro[t * TILE : (t + 1) * TILE, :].T
    tgt_load.wait()
    ids_load.wait()
    gradient(0, g0)

    def pass_on(i):
        remote(xs, xa, xa_s, xa_r, i, two_first).wait_recv()
        remote(xa, xx, xx_s, xx_r, i, down).start()

    with scope("fwdx"):
        for i in range(chunks):
            forward(xs, x_relay, 0, xc, xc_s, xc_r, i)
    with scope("earlyx"):
        early(xs, xc, xc_s, xc_r)
    send_rows(xs, xr, xr_s, xr_r, jnp.logical_or(landing, through))
    for i in range(chunks):
        send_col(g0, gc, gc_s, gc_r, i)
    with scope("passA"):
        for i in range(chunks // 2):
            pass_on(i)

    for i in range(chunks):
        with scope(f"wx{i}"):
            wait_col(xs, xc, xc_s, xc_r, i)
            remote(xs, xr, xr_s, xr_r, i, row_next).wait_recv()

        def first(at, i=i):
            from_col = by_col * xc[i, at, :]
            mixed = own * xs[i, at, :] + by_row * xr[i, at, :] + from_col
            ws[i, at, :] = mixed + from_col
            put(i, at, mixed - STEP * g0[i, at, :])

        over(i, first)
        send_swaps(g0, g_relay, 1, gc_s, i)
        pl.when(inner)(remote(g0, gr, gr_s, gr_r, i, row_next).start)
    send_rows(g0, gr, gr_s, gr_r, direct)
    send_rows(ws, wr, wr_s, wr_r, inner)
    with scope("grad1"):
        gradient(1, g1)

    with scope("passB"):
        for i in range(chunks // 2, chunks):
            pass_on(i)
    with scope("fwdg"):
        for i in range(chunks):
            forward(g0, g_relay, 1, gc, gc_s, gc_r, i)
    with scope("earlyg"):
        early(g0, gc, gc_s, gc_r)
    send_rows(g0, gr, gr_s, gr_r, jnp.logical_or(landing, through))

    for i in range(chunks):
        with scope(f"wg{i}"):
            wait_col(g0, gc, gc_s, gc_r, i)
            remote(g0, gr, gr_s, gr_r, i, row_next).wait_recv()

        def second(at, i=i):
            g = g0[i, at, :]
            mixed = own * g + by_row * gr[i, at, :] + by_col * gc[i, at, :]
            track = (mixed + g1[i, at, :]) - g
            ts[i, at, :] = track
            q[i, at, :] = STEP * (mixed + track)

        over(i, second)
        send_swaps(ts, t_relay, 2, tc_s, i)
        send_col(ts, tc, tc_s, tc_r, i)

    send_rows(ws, wr, wr_s, wr_r, direct)
    send_rows(ts, tr, tr_s, tr_r, jnp.logical_or(direct, inner))
    with scope("fwdt"):
        for i in range(chunks):
            forward(ts, t_relay, 2, tc, tc_s, tc_r, i)
    with scope("earlyt"):
        early(ts, tc, tc_s, tc_r)
    send_rows(ws, wr, wr_s, wr_r, jnp.logical_or(landing, through))
    send_rows(ts, tr, tr_s, tr_r, jnp.logical_or(landing, through))

    for i in range(chunks):
        with scope(f"ww{i}"):
            remote(ws, wr, wr_s, wr_r, i, row_next).wait_recv()
        with scope(f"w2{i}"):
            remote(xa, xx, xx_s, xx_r, i, down).wait_recv()

        def third(at, i=i):
            new = own * ws[i, at, :] + by_row * wr[i, at, :] + (by_col * by_col) * xx[i, at, :] - q[i, at, :]
            put(i, at, new)
            store(xo, i, at, new)

        over(i, third)
    with scope("grad2"):
        gradient(2, q)

    for i in range(chunks):
        with scope(f"wt{i}"):
            wait_col(ts, tc, tc_s, tc_r, i)
            remote(ts, tr, tr_s, tr_r, i, row_next).wait_recv()

        def last(at, i=i):
            mixed = own * ts[i, at, :] + by_row * tr[i, at, :] + by_col * tc[i, at, :]
            store(to, i, at, (mixed + q[i, at, :]) - g1[i, at, :])

        over(i, last)

    with scope("end"):
        for i in range(chunks):
            remote(xs, xc, xc_s, xc_r, i, col_next).wait_send()
            remote(xs, xr, xr_s, xr_r, i, row_next).wait_send()
            remote(xs, xa, xa_s, xa_r, i, two_first).wait_send()
            remote(xa, xx, xx_s, xx_r, i, down).wait_send()
            remote(ws, wr, wr_s, wr_r, i, row_next).wait_send()
            remote(g0, gc, gc_s, gc_r, i, col_next).wait_send()
            remote(g0, gr, gr_s, gr_r, i, row_next).wait_send()
            remote(ts, tc, tc_s, tc_r, i, col_next).wait_send()
            remote(ts, tr, tr_s, tr_r, i, row_next).wait_send()
            if relayed(i):
                @pl.when(seam)
                def _():
                    forward_copy(x_relay, 0, xc, xc_r, i).wait_send()
                    forward_copy(g_relay, 1, gc, gc_r, i).wait_send()
                    forward_copy(t_relay, 2, tc, tc_r, i).wait_send()


def on_device(value_proj, token_pool, target_pool, batch_ids, frozen_out, numerators):
    depth, heads = value_proj.shape[2:]
    n_pool = token_pool.shape[2]
    ids = batch_ids.reshape(batch_ids.shape[2], 1, batch_ids.shape[3])
    chunks, rows = SPLIT * heads // LANES, depth // SPLIT
    field = pltpu.VMEM((chunks, rows, LANES), F32)
    relay = pltpu.VMEM((chunks // 2, rows, LANES), F32)
    dma = pltpu.SemaphoreType.DMA
    out = pltpu.VMEM(value_proj.shape, F32)
    vmem = pl.BlockSpec(memory_space=pltpu.VMEM)
    hbm = pl.BlockSpec(memory_space=pl.ANY)
    return pl.pallas_call(
        kernel,
        out_shape=(out, out),
        in_specs=[
            pl.BlockSpec(memory_space=pltpu.SMEM), hbm, hbm, hbm,
            hbm, hbm,
        ],
        out_specs=(vmem, vmem),
        scratch_shapes=[field] * 15 + [relay] * 3 + [
            pltpu.VMEM((n_pool, depth), BF16),
            pltpu.VMEM((n_pool, depth), BF16),
            pltpu.VMEM((depth, n_pool), BF16),
            pltpu.VMEM((heads, depth), BF16),
            pltpu.VMEM((depth, heads), BF16),
            pltpu.VMEM((n_pool, heads), BF16),
            pltpu.VMEM((depth, heads), BF16),
            pltpu.VMEM(ids.shape, jnp.int32),
            dma((4,)), dma((chunks,)),
        ] + [dma((chunks,))] * 18 + [dma((3, chunks // 2))] * 2,
        compiler_params=pltpu.CompilerParams(
            collective_id=0, has_side_effects=True, vmem_limit_bytes=58 * 2**20,
        ),
    )(numerators, value_proj, token_pool, target_pool, ids, frozen_out)


def solution(mesh):
    return jax.shard_map(
        on_device,
        mesh=mesh,
        in_specs=(
            P("row", "col", None, None),
            P("row", "col", None, None),
            P("row", "col", None, None),
            P("row", "col", None, None),
            P(),
            P(),
        ),
        out_specs=(P("row", "col", None, None), P("row", "col", None, None)),
        check_vma=False,
    )
```

```python
import functools

import jax
import jax.numpy as jnp
from jax import lax
from jax.experimental import pallas as pl
from jax.experimental.pallas import tpu as pltpu
from jax.sharding import PartitionSpec as P

MESH = pl.DeviceIdType.MESH
F32 = jnp.float32
BF16 = jnp.bfloat16
STEP = 0.2
SPLIT = 2
FIRST = 3
ROUND = 4
LANES = 128
TILE = 256


def kernel(
    num_ref, x_hbm, tok_hbm, tgt_hbm, ids_hbm, fro_hbm,
    xo, to,
    xs, xr, xc, xa, xx, ws, wr, g0, gr, gc, g1, ts, tr, tc, q,
    x_relay, g_relay, t_relay, w_relay,
    tok, tgt, tokt, fro, frot, bp, xb, ids_ref,
    load_sem, x_sem,
    xr_s, xr_r, xc_s, xc_r, xa_s, xa_r, xx_s, xx_r, wr_s, wr_r,
    gr_s, gr_r, gc_s, gc_r, tr_s, tr_r, tc_s, tc_r,
    rel_s, rel_r, via_s, via_r,
):
    chunks, rows, _ = xs.shape
    split = tok.shape[1] // rows
    scope = jax.named_scope
    n_pool, depth = tok.shape
    heads = fro.shape[0]
    factor = depth ** -0.5

    r, c = lax.axis_index("row"), lax.axis_index("col")
    y, half = lax.rem(c, 4), 4 * (c // 4)
    seam = y == 3
    plain = jnp.logical_not(seam)
    inner = jnp.logical_or(y == 1, y == 2)
    outer = jnp.logical_not(inner)
    through = jnp.logical_and(seam, lax.rem(r, 4) >= 2)
    landing = y == 0
    direct = jnp.logical_and(seam, jnp.logical_not(through))
    row_next = (lax.rem(r + 1, 16), c)
    row_prev = (lax.rem(r + 15, 16), c)
    col_next = (r, lax.rem(c + 1, 8))
    swap = (r, lax.rem(c + 4, 8))
    up = (r, half + lax.rem(y + 1, 4))
    down = (r, half + lax.rem(y + 3, 4))
    up_swap = (r, lax.rem(up[1] + 4, 8))
    down_swap = (r, lax.rem(down[1] + 4, 8))
    mate = (r, jnp.where(lax.rem(y, 2) == 0, up[1], down[1]))
    mate_next = (row_next[0], mate[1])
    mate_prev = (row_prev[0], mate[1])
    leaves = lax.rem(r, 2) == 1
    two_first = (r, jnp.where(y >= 2, down_swap[1], down[1]))

    def window(ref, i):
        return ref.at[0, 0, pl.ds((i % split) * rows, rows), pl.ds((i // split) * LANES, LANES)]

    loads = [
        pltpu.make_async_copy(window(x_hbm, i), xs.at[i], x_sem.at[i])
        for i in range(chunks)
    ]
    for load in loads:
        load.start()
    tok_load = pltpu.make_async_copy(tok_hbm.at[0, 0], tok, load_sem.at[0])
    fro_load = pltpu.make_async_copy(fro_hbm, fro, load_sem.at[1])
    tgt_load = pltpu.make_async_copy(tgt_hbm.at[0, 0], tgt, load_sem.at[2])
    ids_load = pltpu.make_async_copy(ids_hbm, ids_ref, load_sem.at[3])
    ids_load.start()
    tok_load.start()
    fro_load.start()
    tgt_load.start()

    barrier = pltpu.get_barrier_semaphore()
    partners = (row_next, row_prev, up, down, swap, up_swap, down_swap, mate_next, mate_prev)
    for partner in partners:
        pl.semaphore_signal(barrier, inc=1, device_id=partner, device_id_type=MESH)
    pl.semaphore_wait(barrier, len(partners))

    def remote(src, dst, send, recv, i, device, j=None):
        return pltpu.make_async_remote_copy(
            src_ref=src.at[i], dst_ref=dst.at[i if j is None else j], send_sem=send.at[i],
            recv_sem=recv.at[i], device_id=device, device_id_type=MESH,
        )

    def relayed(i):
        return i % 2 == 1

    def swap_copy(src, relay, which, send, i):
        return pltpu.make_async_remote_copy(
            src_ref=src.at[i], dst_ref=relay.at[i // 2], send_sem=send.at[i],
            recv_sem=rel_r.at[which, i // 2], device_id=swap, device_id_type=MESH,
        )

    def forward_copy(relay, which, dst, recv, i):
        return pltpu.make_async_remote_copy(
            src_ref=relay.at[i // 2], dst_ref=dst.at[i], send_sem=rel_s.at[which, i // 2],
            recv_sem=recv.at[i], device_id=up, device_id_type=MESH,
        )

    def send_swaps(src, relay, which, send, i):
        if relayed(i):
            @pl.when(seam)
            def _():
                swap_copy(src, relay, which, send, i).start()

    def send_col(src, dst, send, recv, i):
        copy = remote(src, dst, send, recv, i, col_next)
        if relayed(i):
            pl.when(jnp.logical_not(seam))(copy.start)
        else:
            copy.start()

    def forward(src, relay, which, dst, send, recv, i):
        if relayed(i):
            @pl.when(seam)
            def _():
                swap_copy(src, relay, which, send, i).wait_recv()
                forward_copy(relay, which, dst, recv, i).start()

    for i in range(chunks):
        loads[i].wait()
        send_swaps(xs, x_relay, 0, xc_s, i)
        send_col(xs, xc, xc_s, xc_r, i)
    def send_rows(src, dst, send, recv, condition=None):
        def go():
            for i in range(chunks):
                remote(src, dst, send, recv, i, row_next).start()

        if condition is None:
            go()
        else:
            pl.when(condition)(go)

    def early(src, dst, send, recv):
        @pl.when(landing)
        def _():
            for i in range(chunks):
                if not relayed(i):
                    remote(src, dst, send, recv, i, col_next).wait_recv()

    def wait_col(src, dst, send, recv, i):
        wait = remote(src, dst, send, recv, i, col_next).wait_recv
        if relayed(i):
            wait()
        else:
            pl.when(jnp.logical_not(landing))(wait)

    send_rows(xs, xr, xr_s, xr_r, jnp.logical_or(inner, direct))
    for i in range(chunks):
        remote(xs, xa, xa_s, xa_r, i, two_first).start()

    weights = [jnp.full((1, LANES), num_ref[i].astype(F32), F32) for i in range(3)]
    total = weights[0] + weights[1] + weights[2]
    own, by_row, by_col = (w / total for w in weights)

    def over(i, body):
        def step(t, carry):
            body(pl.ds(pl.multiple_of(t * LANES, LANES), LANES))
            return carry

        lax.fori_loop(0, rows // LANES, step, 0)

    def gradient(which, out):
        def tile(t, carry):
            at = pl.ds(pl.multiple_of(t * TILE, TILE), TILE)
            pre = jnp.dot(tok[at, :], xb[...], preferred_element_type=F32) * factor
            sig = jax.nn.sigmoid(pre)
            hidden = (pre * sig).astype(BF16)
            slope = sig * (1.0 + pre * (1.0 - sig))
            output = jnp.dot(hidden, fro[...], preferred_element_type=F32)
            err = (output - tgt[at, :].astype(F32)).astype(BF16)
            back = jnp.dot(err, frot[...], preferred_element_type=F32)
            place = t * TILE + lax.broadcasted_iota(jnp.int32, (TILE, LANES), 0)
            drawn = jnp.zeros((TILE, LANES), F32)
            for l in range(ids_ref.shape[2] // LANES):
                ids = ids_ref[which, :, l * LANES : (l + 1) * LANES]
                drawn += jnp.where(ids == place, 1.0, 0.0)
            drawn = jnp.sum(drawn, axis=1, keepdims=True)
            bp[at, :] = (back * slope * drawn).astype(BF16)
            return carry

        lax.fori_loop(0, n_pool // TILE, tile, 0)

        def block(t, carry):
            to = pl.ds(pl.multiple_of(t * TILE, TILE), TILE)
            for p in range(split):
                at = pl.ds(pl.multiple_of(t * TILE + p * rows, TILE), TILE)
                for n in range(heads // TILE):
                    g = jnp.dot(tokt[at, :], bp[:, n * TILE : (n + 1) * TILE], preferred_element_type=F32) * factor
                    for l in range(TILE // LANES):
                        out[(n * (TILE // LANES) + l) * split + p, to, :] = g[:, l * LANES : (l + 1) * LANES]
            return carry

        lax.fori_loop(0, rows // TILE, block, 0)

    def store(ref, i, at, value):
        to_rows = pl.ds(at.start + (i % split) * rows, LANES)
        ref[0, 0, to_rows, (i // split) * LANES : (i // split + 1) * LANES] = value

    def put(i, at, value):
        to = pl.ds(at.start + (i % split) * rows, LANES)
        xb[to, (i // split) * LANES : (i // split + 1) * LANES] = value.astype(BF16)

    for i in range(chunks):
        def cast(at, i=i):
            put(i, at, xs[i, at, :])
        over(i, cast)
    tok_load.wait()

    def turn(t, carry):
        at = pl.ds(pl.multiple_of(t * TILE, TILE), TILE)
        tokt[:, at] = tok[at, :].T
        return carry

    lax.fori_loop(0, n_pool // TILE, turn, 0)
    fro_load.wait()
    for t in range(heads // TILE):
        frot[:, t * TILE : (t + 1) * TILE] = fro[t * TILE : (t + 1) * TILE, :].T
    tgt_load.wait()
    ids_load.wait()
    gradient(0, g0)

    def via_copy(i):
        return pltpu.make_async_remote_copy(
            src_ref=ws.at[i], dst_ref=w_relay.at[i], send_sem=wr_s.at[i],
            recv_sem=via_r.at[i], device_id=mate_next, device_id_type=MESH,
        )

    def via_forward(i):
        return pltpu.make_async_remote_copy(
            src_ref=w_relay.at[i], dst_ref=wr.at[i], send_sem=via_s.at[i],
            recv_sem=wr_r.at[i], device_id=mate, device_id_type=MESH,
        )

    around = jnp.logical_and(outer, leaves)
    carries = jnp.logical_and(inner, jnp.logical_not(leaves))

    def send_around():
        @pl.when(around)
        def _():
            for i in range(ROUND):
                via_copy(i).start()

    def carry_on():
        @pl.when(carries)
        def _():
            for i in range(ROUND):
                via_copy(i).wait_recv()
                via_forward(i).start()

    def send_rest(condition):
        @pl.when(condition)
        def _():
            for i in range(ROUND):
                pl.when(jnp.logical_not(around))(remote(ws, wr, wr_s, wr_r, i, row_next).start)
            for i in range(ROUND, chunks):
                remote(ws, wr, wr_s, wr_r, i, row_next).start()

    def pass_on(i):
        remote(xs, xa, xa_s, xa_r, i, two_first).wait_recv()
        remote(xa, xx, xx_s, xx_r, i, down).start()

    with scope("fwdx"):
        for i in range(chunks):
            forward(xs, x_relay, 0, xc, xc_s, xc_r, i)
    with scope("earlyx"):
        early(xs, xc, xc_s, xc_r)
    send_rows(xs, xr, xr_s, xr_r, jnp.logical_or(landing, through))
    for i in range(chunks):
        send_col(g0, gc, gc_s, gc_r, i)
    with scope("passA"):
        for i in range(chunks // 2):
            pass_on(i)

    for i in range(chunks):
        with scope(f"wx{i}"):
            wait_col(xs, xc, xc_s, xc_r, i)
            remote(xs, xr, xr_s, xr_r, i, row_next).wait_recv()

        def first(at, i=i):
            from_col = by_col * xc[i, at, :]
            mixed = own * xs[i, at, :] + by_row * xr[i, at, :] + from_col
            ws[i, at, :] = mixed + from_col
            put(i, at, mixed - STEP * g0[i, at, :])

        over(i, first)
        send_swaps(g0, g_relay, 1, gc_s, i)
        pl.when(inner)(remote(g0, gr, gr_s, gr_r, i, row_next).start)
    send_rows(g0, gr, gr_s, gr_r, direct)
    with scope("grad1"):
        gradient(1, g1)

    with scope("passB"):
        for i in range(chunks // 2, chunks):
            pass_on(i)
    with scope("fwdg"):
        for i in range(chunks):
            forward(g0, g_relay, 1, gc, gc_s, gc_r, i)
    with scope("earlyg"):
        early(g0, gc, gc_s, gc_r)
    send_rows(g0, gr, gr_s, gr_r, jnp.logical_or(landing, through))
    send_around()

    for i in range(chunks):
        with scope(f"wg{i}"):
            wait_col(g0, gc, gc_s, gc_r, i)
            remote(g0, gr, gr_s, gr_r, i, row_next).wait_recv()

        def second(at, i=i):
            g = g0[i, at, :]
            mixed = own * g + by_row * gr[i, at, :] + by_col * gc[i, at, :]
            track = (mixed + g1[i, at, :]) - g
            ts[i, at, :] = track
            q[i, at, :] = STEP * (mixed + track)

        over(i, second)
        send_swaps(ts, t_relay, 2, tc_s, i)
        if i < FIRST:
            send_col(ts, tc, tc_s, tc_r, i)
        else:
            @pl.when(outer)
            def _(i=i):
                send_col(ts, tc, tc_s, tc_r, i)


    send_rest(jnp.logical_or(direct, landing))
    send_rows(ws, wr, wr_s, wr_r, inner)
    send_rows(ts, tr, tr_s, tr_r, jnp.logical_or(direct, inner))
    with scope("fwdt"):
        for i in range(chunks):
            forward(ts, t_relay, 2, tc, tc_s, tc_r, i)
    with scope("earlyt"):
        early(ts, tc, tc_s, tc_r)
    send_rest(through)
    send_rows(ts, tr, tr_s, tr_r, jnp.logical_or(landing, through))

    with scope("carry"):
        carry_on()

    @pl.when(inner)
    def _():
        for i in range(FIRST, chunks):
            send_col(ts, tc, tc_s, tc_r, i)

    for i in range(chunks):
        with scope(f"ww{i}"):
            remote(ws, wr, wr_s, wr_r, i, row_next).wait_recv()
        with scope(f"w2{i}"):
            remote(xa, xx, xx_s, xx_r, i, down).wait_recv()

        def third(at, i=i):
            new = own * ws[i, at, :] + by_row * wr[i, at, :] + (by_col * by_col) * xx[i, at, :] - q[i, at, :]
            put(i, at, new)
            store(xo, i, at, new)

        over(i, third)
    with scope("grad2"):
        gradient(2, q)

    for i in range(chunks):
        with scope(f"wt{i}"):
            wait_col(ts, tc, tc_s, tc_r, i)
            remote(ts, tr, tr_s, tr_r, i, row_next).wait_recv()

        def last(at, i=i):
            mixed = own * ts[i, at, :] + by_row * tr[i, at, :] + by_col * tc[i, at, :]
            store(to, i, at, (mixed + q[i, at, :]) - g1[i, at, :])

        over(i, last)

    with scope("end"):
        for i in range(chunks):
            remote(xs, xc, xc_s, xc_r, i, col_next).wait_send()
            remote(xs, xr, xr_s, xr_r, i, row_next).wait_send()
            remote(xs, xa, xa_s, xa_r, i, two_first).wait_send()
            remote(xa, xx, xx_s, xx_r, i, down).wait_send()
            remote(ws, wr, wr_s, wr_r, i, row_next).wait_send()
            remote(g0, gc, gc_s, gc_r, i, col_next).wait_send()
            remote(g0, gr, gr_s, gr_r, i, row_next).wait_send()
            remote(ts, tc, tc_s, tc_r, i, col_next).wait_send()
            remote(ts, tr, tr_s, tr_r, i, row_next).wait_send()
            if relayed(i):
                @pl.when(seam)
                def _():
                    forward_copy(x_relay, 0, xc, xc_r, i).wait_send()
                    forward_copy(g_relay, 1, gc, gc_r, i).wait_send()
                    forward_copy(t_relay, 2, tc, tc_r, i).wait_send()

        @pl.when(carries)
        def _():
            for i in range(ROUND):
                via_forward(i).wait_send()


def on_device(value_proj, token_pool, target_pool, batch_ids, frozen_out, numerators):
    depth, heads = value_proj.shape[2:]
    n_pool = token_pool.shape[2]
    ids = batch_ids.reshape(batch_ids.shape[2], 1, batch_ids.shape[3])
    chunks, rows = SPLIT * heads // LANES, depth // SPLIT
    field = pltpu.VMEM((chunks, rows, LANES), F32)
    relay = pltpu.VMEM((chunks // 2, rows, LANES), F32)
    dma = pltpu.SemaphoreType.DMA
    out = pltpu.VMEM(value_proj.shape, F32)
    vmem = pl.BlockSpec(memory_space=pltpu.VMEM)
    hbm = pl.BlockSpec(memory_space=pl.ANY)
    return pl.pallas_call(
        kernel,
        out_shape=(out, out),
        in_specs=[
            pl.BlockSpec(memory_space=pltpu.SMEM), hbm, hbm, hbm,
            hbm, hbm,
        ],
        out_specs=(vmem, vmem),
        scratch_shapes=[field] * 15 + [relay] * 3 + [
            pltpu.VMEM((ROUND, rows, LANES), F32),
            pltpu.VMEM((n_pool, depth), BF16),
            pltpu.VMEM((n_pool, depth), BF16),
            pltpu.VMEM((depth, n_pool), BF16),
            pltpu.VMEM((heads, depth), BF16),
            pltpu.VMEM((depth, heads), BF16),
            pltpu.VMEM((n_pool, heads), BF16),
            pltpu.VMEM((depth, heads), BF16),
            pltpu.VMEM(ids.shape, jnp.int32),
            dma((4,)), dma((chunks,)),
        ] + [dma((chunks,))] * 18 + [dma((3, chunks // 2))] * 2 + [dma((ROUND,))] * 2,
        compiler_params=pltpu.CompilerParams(
            collective_id=0, has_side_effects=True, vmem_limit_bytes=58 * 2**20,
        ),
    )(numerators, value_proj, token_pool, target_pool, ids, frozen_out)


def solution(mesh):
    return jax.shard_map(
        on_device,
        mesh=mesh,
        in_specs=(
            P("row", "col", None, None),
            P("row", "col", None, None),
            P("row", "col", None, None),
            P("row", "col", None, None),
            P(),
            P(),
        ),
        out_specs=(P("row", "col", None, None), P("row", "col", None, None)),
        check_vma=False,
    )
```

```python
import functools

import jax
import jax.numpy as jnp
from jax import lax
from jax.experimental import pallas as pl
from jax.experimental.pallas import tpu as pltpu
from jax.sharding import PartitionSpec as P

MESH = pl.DeviceIdType.MESH
F32 = jnp.float32
BF16 = jnp.bfloat16
STEP = 0.2
SPLIT = 2
AHEAD = 6
BEHIND = 7
FIRST = 3
ROUND = 5
LANES = 128
TILE = 256


def kernel(
    num_ref, x_hbm, tok_hbm, tgt_hbm, ids_hbm, fro_hbm,
    xo, to,
    xs, xr, xc, xa, xx, ws, wr, g0, gr, gc, g1, ts, tr, tc, q,
    x_relay, g_relay, t_relay, w_relay,
    tok, tgt, tokt, fro, frot, bp, xb, ids_ref,
    load_sem, x_sem,
    xr_s, xr_r, xc_s, xc_r, xa_s, xa_r, xx_s, xx_r, wr_s, wr_r,
    gr_s, gr_r, gc_s, gc_r, tr_s, tr_r, tc_s, tc_r,
    rel_s, rel_r, via_s, via_r,
):
    chunks, rows, _ = xs.shape
    split = tok.shape[1] // rows
    scope = jax.named_scope
    n_pool, depth = tok.shape
    heads = fro.shape[0]
    factor = depth ** -0.5

    r, c = lax.axis_index("row"), lax.axis_index("col")
    y, half = lax.rem(c, 4), 4 * (c // 4)
    seam = y == 3
    plain = jnp.logical_not(seam)
    inner = jnp.logical_or(y == 1, y == 2)
    outer = jnp.logical_not(inner)
    through = jnp.logical_and(seam, lax.rem(r, 4) >= 2)
    landing = y == 0
    direct = jnp.logical_and(seam, jnp.logical_not(through))
    row_next = (lax.rem(r + 1, 16), c)
    row_prev = (lax.rem(r + 15, 16), c)
    col_next = (r, lax.rem(c + 1, 8))
    swap = (r, lax.rem(c + 4, 8))
    up = (r, half + lax.rem(y + 1, 4))
    down = (r, half + lax.rem(y + 3, 4))
    up_swap = (r, lax.rem(up[1] + 4, 8))
    down_swap = (r, lax.rem(down[1] + 4, 8))
    mate = (r, jnp.where(lax.rem(y, 2) == 0, up[1], down[1]))
    mate_next = (row_next[0], mate[1])
    mate_prev = (row_prev[0], mate[1])
    leaves = lax.rem(r, 2) == 1
    two_first = (r, jnp.where(y >= 2, down_swap[1], down[1]))

    def window(ref, i):
        return ref.at[0, 0, pl.ds((i % split) * rows, rows), pl.ds((i // split) * LANES, LANES)]

    loads = [
        pltpu.make_async_copy(window(x_hbm, i), xs.at[i], x_sem.at[i])
        for i in range(chunks)
    ]
    for load in loads:
        load.start()
    tok_load = pltpu.make_async_copy(tok_hbm.at[0, 0], tok, load_sem.at[0])
    fro_load = pltpu.make_async_copy(fro_hbm, fro, load_sem.at[1])
    tgt_load = pltpu.make_async_copy(tgt_hbm.at[0, 0], tgt, load_sem.at[2])
    ids_load = pltpu.make_async_copy(ids_hbm, ids_ref, load_sem.at[3])
    ids_load.start()
    tok_load.start()
    fro_load.start()
    tgt_load.start()

    barrier = pltpu.get_barrier_semaphore()
    partners = (row_next, row_prev, up, down, swap, up_swap, down_swap, mate_next, mate_prev)
    for partner in partners:
        pl.semaphore_signal(barrier, inc=1, device_id=partner, device_id_type=MESH)
    pl.semaphore_wait(barrier, len(partners))

    def remote(src, dst, send, recv, i, device, j=None):
        return pltpu.make_async_remote_copy(
            src_ref=src.at[i], dst_ref=dst.at[i if j is None else j], send_sem=send.at[i],
            recv_sem=recv.at[i], device_id=device, device_id_type=MESH,
        )

    def relayed(i):
        return i % 2 == 1

    def swap_copy(src, relay, which, send, i):
        return pltpu.make_async_remote_copy(
            src_ref=src.at[i], dst_ref=relay.at[i // 2], send_sem=send.at[i],
            recv_sem=rel_r.at[which, i // 2], device_id=swap, device_id_type=MESH,
        )

    def forward_copy(relay, which, dst, recv, i):
        return pltpu.make_async_remote_copy(
            src_ref=relay.at[i // 2], dst_ref=dst.at[i], send_sem=rel_s.at[which, i // 2],
            recv_sem=recv.at[i], device_id=up, device_id_type=MESH,
        )

    def send_swaps(src, relay, which, send, i):
        if relayed(i):
            @pl.when(seam)
            def _():
                swap_copy(src, relay, which, send, i).start()

    def send_col(src, dst, send, recv, i):
        copy = remote(src, dst, send, recv, i, col_next)
        if relayed(i):
            pl.when(jnp.logical_not(seam))(copy.start)
        else:
            copy.start()

    def forward(src, relay, which, dst, send, recv, i):
        if relayed(i):
            @pl.when(seam)
            def _():
                swap_copy(src, relay, which, send, i).wait_recv()
                forward_copy(relay, which, dst, recv, i).start()

    for i in range(chunks):
        loads[i].wait()
        send_swaps(xs, x_relay, 0, xc_s, i)
        send_col(xs, xc, xc_s, xc_r, i)
    def send_rows(src, dst, send, recv, condition=None):
        def go():
            for i in range(chunks):
                remote(src, dst, send, recv, i, row_next).start()

        if condition is None:
            go()
        else:
            pl.when(condition)(go)

    def early(src, dst, send, recv):
        @pl.when(landing)
        def _():
            for i in range(chunks):
                if i < AHEAD and not relayed(i):
                    remote(src, dst, send, recv, i, col_next).wait_recv()

    def wait_col(src, dst, send, recv, i):
        wait = remote(src, dst, send, recv, i, col_next).wait_recv
        if relayed(i) or i >= AHEAD:
            wait()
        else:
            pl.when(jnp.logical_not(landing))(wait)

    send_rows(xs, xr, xr_s, xr_r, jnp.logical_or(inner, direct))
    for i in range(chunks // 2):
        remote(xs, xa, xa_s, xa_r, i, two_first).start()

    weights = [jnp.full((1, LANES), num_ref[i].astype(F32), F32) for i in range(3)]
    total = weights[0] + weights[1] + weights[2]
    own, by_row, by_col = (w / total for w in weights)

    def over(i, body):
        def step(t, carry):
            body(pl.ds(pl.multiple_of(t * LANES, LANES), LANES))
            return carry

        lax.fori_loop(0, rows // LANES, step, 0)

    def gradient(which, out):
        def tile(t, carry):
            at = pl.ds(pl.multiple_of(t * TILE, TILE), TILE)
            pre = jnp.dot(tok[at, :], xb[...], preferred_element_type=F32) * factor
            sig = jax.nn.sigmoid(pre)
            hidden = (pre * sig).astype(BF16)
            slope = sig * (1.0 + pre * (1.0 - sig))
            output = jnp.dot(hidden, fro[...], preferred_element_type=F32)
            err = (output - tgt[at, :].astype(F32)).astype(BF16)
            back = jnp.dot(err, frot[...], preferred_element_type=F32)
            place = t * TILE + lax.broadcasted_iota(jnp.int32, (TILE, LANES), 0)
            drawn = jnp.zeros((TILE, LANES), F32)
            for l in range(ids_ref.shape[2] // LANES):
                ids = ids_ref[which, :, l * LANES : (l + 1) * LANES]
                drawn += jnp.where(ids == place, 1.0, 0.0)
            drawn = jnp.sum(drawn, axis=1, keepdims=True)
            bp[at, :] = (back * slope * drawn).astype(BF16)
            return carry

        lax.fori_loop(0, n_pool // TILE, tile, 0)

        def block(t, carry):
            to = pl.ds(pl.multiple_of(t * TILE, TILE), TILE)
            for p in range(split):
                at = pl.ds(pl.multiple_of(t * TILE + p * rows, TILE), TILE)
                for n in range(heads // TILE):
                    g = jnp.dot(tokt[at, :], bp[:, n * TILE : (n + 1) * TILE], preferred_element_type=F32) * factor
                    for l in range(TILE // LANES):
                        out[(n * (TILE // LANES) + l) * split + p, to, :] = g[:, l * LANES : (l + 1) * LANES]
            return carry

        lax.fori_loop(0, rows // TILE, block, 0)

    def store(ref, i, at, value):
        to_rows = pl.ds(at.start + (i % split) * rows, LANES)
        ref[0, 0, to_rows, (i // split) * LANES : (i // split + 1) * LANES] = value

    def put(i, at, value):
        to = pl.ds(at.start + (i % split) * rows, LANES)
        xb[to, (i // split) * LANES : (i // split + 1) * LANES] = value.astype(BF16)

    for i in range(chunks):
        def cast(at, i=i):
            put(i, at, xs[i, at, :])
        over(i, cast)
    tok_load.wait()

    def turn(t, carry):
        at = pl.ds(pl.multiple_of(t * TILE, TILE), TILE)
        tokt[:, at] = tok[at, :].T
        return carry

    lax.fori_loop(0, n_pool // TILE, turn, 0)
    fro_load.wait()
    for t in range(heads // TILE):
        frot[:, t * TILE : (t + 1) * TILE] = fro[t * TILE : (t + 1) * TILE, :].T
    tgt_load.wait()
    ids_load.wait()
    gradient(0, g0)

    def via_copy(i):
        return pltpu.make_async_remote_copy(
            src_ref=ws.at[i], dst_ref=w_relay.at[i], send_sem=wr_s.at[i],
            recv_sem=via_r.at[i], device_id=mate_next, device_id_type=MESH,
        )

    def via_forward(i):
        return pltpu.make_async_remote_copy(
            src_ref=w_relay.at[i], dst_ref=wr.at[i], send_sem=via_s.at[i],
            recv_sem=wr_r.at[i], device_id=mate, device_id_type=MESH,
        )

    around = jnp.logical_and(outer, leaves)
    carries = jnp.logical_and(inner, jnp.logical_not(leaves))

    def send_around():
        @pl.when(around)
        def _():
            for i in range(ROUND):
                via_copy(i).start()

    def carry_on():
        @pl.when(carries)
        def _():
            for i in range(ROUND):
                via_copy(i).wait_recv()
                via_forward(i).start()

    def send_rest(condition):
        @pl.when(condition)
        def _():
            for i in range(ROUND):
                pl.when(jnp.logical_not(around))(remote(ws, wr, wr_s, wr_r, i, row_next).start)
            for i in range(ROUND, chunks):
                remote(ws, wr, wr_s, wr_r, i, row_next).start()

    def pass_on(i):
        remote(xs, xa, xa_s, xa_r, i, two_first).wait_recv()
        remote(xa, xx, xx_s, xx_r, i, down).start()

    with scope("fwdx"):
        for i in range(chunks):
            forward(xs, x_relay, 0, xc, xc_s, xc_r, i)
            if i == BEHIND:
                send_rows(xs, xr, xr_s, xr_r, through)
    with scope("earlyx"):
        early(xs, xc, xc_s, xc_r)
    send_rows(xs, xr, xr_s, xr_r, landing)
    for i in range(chunks):
        send_col(g0, gc, gc_s, gc_r, i)
    with scope("passA"):
        for i in range(chunks // 2):
            pass_on(i)
    for i in range(chunks // 2, chunks):
        remote(xs, xa, xa_s, xa_r, i, two_first).start()

    for i in range(chunks):
        with scope(f"wx{i}"):
            wait_col(xs, xc, xc_s, xc_r, i)
            remote(xs, xr, xr_s, xr_r, i, row_next).wait_recv()

        def first(at, i=i):
            from_col = by_col * xc[i, at, :]
            mixed = own * xs[i, at, :] + by_row * xr[i, at, :] + from_col
            ws[i, at, :] = mixed + from_col
            put(i, at, mixed - STEP * g0[i, at, :])

        over(i, first)
        send_swaps(g0, g_relay, 1, gc_s, i)
        pl.when(inner)(remote(g0, gr, gr_s, gr_r, i, row_next).start)
    send_rows(g0, gr, gr_s, gr_r, direct)
    with scope("grad1"):
        gradient(1, g1)

    with scope("fwdg"):
        for i in range(chunks):
            forward(g0, g_relay, 1, gc, gc_s, gc_r, i)
            if i == BEHIND:
                send_rows(g0, gr, gr_s, gr_r, through)
    with scope("earlyg"):
        early(g0, gc, gc_s, gc_r)
    send_rows(g0, gr, gr_s, gr_r, landing)
    send_around()
    with scope("passB"):
        for i in range(chunks // 2, chunks):
            pass_on(i)

    for i in range(chunks):
        with scope(f"wg{i}"):
            wait_col(g0, gc, gc_s, gc_r, i)
            remote(g0, gr, gr_s, gr_r, i, row_next).wait_recv()

        def second(at, i=i):
            g = g0[i, at, :]
            mixed = own * g + by_row * gr[i, at, :] + by_col * gc[i, at, :]
            track = (mixed + g1[i, at, :]) - g
            ts[i, at, :] = track
            q[i, at, :] = STEP * (mixed + track)

        over(i, second)
        send_swaps(ts, t_relay, 2, tc_s, i)
        if i < FIRST:
            send_col(ts, tc, tc_s, tc_r, i)
        else:
            @pl.when(outer)
            def _(i=i):
                send_col(ts, tc, tc_s, tc_r, i)


    send_rest(jnp.logical_or(direct, landing))
    send_rows(ws, wr, wr_s, wr_r, inner)
    send_rows(ts, tr, tr_s, tr_r, jnp.logical_or(direct, inner))
    with scope("fwdt"):
        for i in range(chunks):
            forward(ts, t_relay, 2, tc, tc_s, tc_r, i)
            if i == BEHIND:
                send_rest(through)
                send_rows(ts, tr, tr_s, tr_r, through)
    with scope("earlyt"):
        early(ts, tc, tc_s, tc_r)
    send_rows(ts, tr, tr_s, tr_r, landing)

    with scope("carry"):
        carry_on()

    @pl.when(inner)
    def _():
        for i in range(FIRST, chunks):
            send_col(ts, tc, tc_s, tc_r, i)

    for i in range(chunks):
        with scope(f"ww{i}"):
            remote(ws, wr, wr_s, wr_r, i, row_next).wait_recv()
        with scope(f"w2{i}"):
            remote(xa, xx, xx_s, xx_r, i, down).wait_recv()

        def third(at, i=i):
            new = own * ws[i, at, :] + by_row * wr[i, at, :] + (by_col * by_col) * xx[i, at, :] - q[i, at, :]
            put(i, at, new)
            store(xo, i, at, new)

        over(i, third)
    with scope("grad2"):
        gradient(2, q)

    for i in range(chunks):
        with scope(f"wt{i}"):
            wait_col(ts, tc, tc_s, tc_r, i)
            remote(ts, tr, tr_s, tr_r, i, row_next).wait_recv()

        def last(at, i=i):
            mixed = own * ts[i, at, :] + by_row * tr[i, at, :] + by_col * tc[i, at, :]
            store(to, i, at, (mixed + q[i, at, :]) - g1[i, at, :])

        over(i, last)

    with scope("end"):
        for i in range(chunks):
            remote(xs, xc, xc_s, xc_r, i, col_next).wait_send()
            remote(xs, xr, xr_s, xr_r, i, row_next).wait_send()
            remote(xs, xa, xa_s, xa_r, i, two_first).wait_send()
            remote(xa, xx, xx_s, xx_r, i, down).wait_send()
            remote(ws, wr, wr_s, wr_r, i, row_next).wait_send()
            remote(g0, gc, gc_s, gc_r, i, col_next).wait_send()
            remote(g0, gr, gr_s, gr_r, i, row_next).wait_send()
            remote(ts, tc, tc_s, tc_r, i, col_next).wait_send()
            remote(ts, tr, tr_s, tr_r, i, row_next).wait_send()
            if relayed(i):
                @pl.when(seam)
                def _():
                    forward_copy(x_relay, 0, xc, xc_r, i).wait_send()
                    forward_copy(g_relay, 1, gc, gc_r, i).wait_send()
                    forward_copy(t_relay, 2, tc, tc_r, i).wait_send()

        @pl.when(carries)
        def _():
            for i in range(ROUND):
                via_forward(i).wait_send()


def on_device(value_proj, token_pool, target_pool, batch_ids, frozen_out, numerators):
    depth, heads = value_proj.shape[2:]
    n_pool = token_pool.shape[2]
    ids = batch_ids.reshape(batch_ids.shape[2], 1, batch_ids.shape[3])
    chunks, rows = SPLIT * heads // LANES, depth // SPLIT
    field = pltpu.VMEM((chunks, rows, LANES), F32)
    relay = pltpu.VMEM((chunks // 2, rows, LANES), F32)
    dma = pltpu.SemaphoreType.DMA
    out = pltpu.VMEM(value_proj.shape, F32)
    vmem = pl.BlockSpec(memory_space=pltpu.VMEM)
    hbm = pl.BlockSpec(memory_space=pl.ANY)
    return pl.pallas_call(
        kernel,
        out_shape=(out, out),
        in_specs=[
            pl.BlockSpec(memory_space=pltpu.SMEM), hbm, hbm, hbm,
            hbm, hbm,
        ],
        out_specs=(vmem, vmem),
        scratch_shapes=[field] * 15 + [relay] * 3 + [
            pltpu.VMEM((ROUND, rows, LANES), F32),
            pltpu.VMEM((n_pool, depth), BF16),
            pltpu.VMEM((n_pool, depth), BF16),
            pltpu.VMEM((depth, n_pool), BF16),
            pltpu.VMEM((heads, depth), BF16),
            pltpu.VMEM((depth, heads), BF16),
            pltpu.VMEM((n_pool, heads), BF16),
            pltpu.VMEM((depth, heads), BF16),
            pltpu.VMEM(ids.shape, jnp.int32),
            dma((4,)), dma((chunks,)),
        ] + [dma((chunks,))] * 18 + [dma((3, chunks // 2))] * 2 + [dma((ROUND,))] * 2,
        compiler_params=pltpu.CompilerParams(
            collective_id=0, has_side_effects=True, vmem_limit_bytes=58 * 2**20,
        ),
    )(numerators, value_proj, token_pool, target_pool, ids, frozen_out)


def solution(mesh):
    return jax.shard_map(
        on_device,
        mesh=mesh,
        in_specs=(
            P("row", "col", None, None),
            P("row", "col", None, None),
            P("row", "col", None, None),
            P("row", "col", None, None),
            P(),
            P(),
        ),
        out_specs=(P("row", "col", None, None), P("row", "col", None, None)),
        check_vma=False,
    )
```
